32 devices in a mesh: ta: 4 (over z), gz: 2 (over x), xy: 4 (over y, core).
Axes of the slice: x: 2, y: 2, z: 4, core: 2. Of those that a mesh axis runs over, the one named last changes fastest.
Arguments:
- links: float32 [4, 2, 4, 4, 9, 4608], P('ta', 'gz', 'xy'), may hold values from -1 to 3
- eigvecs: float32 [4, 2, 4, 4, 48, 128], P('ta', 'gz', 'xy'), may hold values from -1 to 1
- eig_real: float32 [64], replicated, may hold values from 0.8 to 2.5
- eig_imag: float32 [64], replicated, may hold values from -0.5 to 0.5
- rhs: float32 [4, 2, 4, 4, 48, 128], P('ta', 'gz', 'xy'), may hold values from -3000 to 3000
Outputs:
- solution: float32 [4, 2, 4, 4, 48, 128], P('ta', 'gz', 'xy')
- residual: float32 [4, 2, 4, 4, 48, 128], P('ta', 'gz', 'xy')
The draws below stay inside these ranges and needn't reach their ends.
All inputs are finite; a program needn't handle non-finite values.
Results may differ from the reference program's by a relative error of at most 0.0003.
Values sent between devices are 32-bit elements; how exact they have to be, the bound alone decides.
No kernel may reach another device: no remote copies, remote signals or barrier semaphores. Data moves between devices by JAX's collectives and lax.ppermute only.
A program may use at most 64 MiB of HBM per device.

```python
import jax
import jax.numpy as jnp
from jax import lax

DOF = 48
NEV = 64
NRHS = 64
SWEEPS = 4
NT = 4
NZ = 2
NX = 4
NY = 4


def eigen_fields(key):
    shape = (NT, NZ, NX, NY, DOF, 2 * NEV)
    values = jnp.clip(jax.random.normal(key, shape, jnp.float32), -4.0, 4.0)
    return values / jnp.sqrt(jnp.float32(NT * NZ * NX * NY * DOF * 2))


def draw_eigvecs(key, part):
    return eigen_fields(jax.random.fold_in(key, 7))


def draw_rhs(key, part):
    vectors = eigen_fields(jax.random.fold_in(key, 7))
    keys = jax.random.split(jax.random.fold_in(key, 13), 4)
    spread = jnp.sqrt(jnp.float32(NT * NZ * NX * NY * DOF * 2) / jnp.float32(2 * NEV))
    weights = jnp.clip(jax.random.normal(keys[0], (2 * NEV, NRHS), jnp.float32), -4.0, 4.0) * spread
    w_re = weights[:NEV]
    w_im = weights[NEV:]
    block = jnp.concatenate([jnp.concatenate([w_re, w_im], 1), jnp.concatenate([-w_im, w_re], 1)], 0)
    along = jnp.einsum('tzxydk,kc->tzxydc', vectors, block, precision=lax.Precision.HIGHEST)
    site_scale = jnp.exp(jax.random.uniform(keys[1], (NT, NZ, NX, NY, 1, 1), jnp.float32, 0.0, 2.3026))
    column = jnp.exp(jax.random.uniform(keys[2], (NRHS,), jnp.float32, 0.0, 2.3026))
    column = jnp.concatenate([column, column])
    ramp_t = 3.0 ** (jnp.arange(NT, dtype=jnp.float32) / max(NT - 1, 1))
    ramp_z = 3.0 ** (jnp.arange(NZ, dtype=jnp.float32) / max(NZ - 1, 1))
    ramp_x = 3.0 ** (jnp.arange(NX, dtype=jnp.float32) / max(NX - 1, 1))
    ramp = ramp_t[:, None, None] * ramp_z[None, :, None] * ramp_x[None, None, :]
    ramp = ramp[:, :, :, None, None, None]
    shape = (NT, NZ, NX, NY, DOF, 2 * NRHS)
    noise = jnp.clip(jax.random.normal(keys[3], shape, jnp.float32), -4.0, 4.0)
    return along + noise * site_scale * column * ramp / 30.0


def draw_links(key, part):
    keys = jax.random.split(jax.random.fold_in(key, 21), 2)
    shape = (NT, NZ, NX, NY, 9, DOF, 2 * DOF)
    noise = jnp.clip(jax.random.normal(keys[0], shape, jnp.float32), -4.0, 4.0)
    own = (jnp.arange(9) == 0).astype(jnp.float32)
    factor = 0.01 + 0.01 * own
    noise = noise * factor[:, None, None]
    mass = jax.random.uniform(keys[1], (NT, NZ, NX, NY, 1, 1, 1), jnp.float32, 1.0, 2.5)
    identity = jnp.eye(DOF, 2 * DOF, dtype=jnp.float32)
    full = noise + mass * identity[None, :, :] * own[:, None, None]
    return full.reshape(NT, NZ, NX, NY, 9, 2 * DOF * DOF)


def setup_inputs(seed: int = 0) -> dict:
    streams_of = jax.random.split(jax.random.key(seed), 6)
    links = draw_links(jax.random.fold_in(streams_of[5], 71), 0)
    eigvecs = draw_eigvecs(jax.random.fold_in(streams_of[5], 71), 0)
    eig_real = jnp.clip(jax.random.uniform(streams_of[2], (NEV,), jnp.float32, 0.8, 2.5), 0.8, 2.5)
    eig_imag = jnp.clip(jax.random.uniform(streams_of[3], (NEV,), jnp.float32, -0.5, 0.5), -0.5, 0.5)
    rhs = draw_rhs(jax.random.fold_in(streams_of[5], 71), 0)
    return {"links": links, "eigvecs": eigvecs, "eig_real": eig_real, "eig_imag": eig_imag, "rhs": rhs}


HIGH = lax.Precision.HIGHEST


def link_apply(matrix, field):
    half = field.shape[-1] // 2
    real = jnp.einsum('tzxyoi,tzxyic->tzxyoc', matrix[..., :DOF], field, precision=HIGH)
    imag = jnp.einsum('tzxyoi,tzxyic->tzxyoc', matrix[..., DOF:], field, precision=HIGH)
    return jnp.concatenate([real[..., :half] - imag[..., half:], real[..., half:] + imag[..., :half]], -1)


def operate(links, field):
    total = link_apply(links[:, :, :, :, 0], field)
    for axis in range(4):
        total = total - link_apply(links[:, :, :, :, 1 + axis], jnp.roll(field, -1, axis))
        total = total - link_apply(links[:, :, :, :, 5 + axis], jnp.roll(field, 1, axis))
    return total


def complex_scale(alpha_re, alpha_im, field):
    half = field.shape[-1] // 2
    f_re = field[..., :half]
    f_im = field[..., half:]
    return jnp.concatenate([alpha_re * f_re - alpha_im * f_im, alpha_re * f_im + alpha_im * f_re], -1)


def reference(links, eigvecs, eig_real, eig_imag, rhs):
    links = links.reshape(NT, NZ, NX, NY, 9, DOF, 2 * DOF)
    rows = eigvecs.reshape(-1, 2 * NEV)
    cross = jnp.dot(rows.T, rhs.reshape(-1, 2 * NRHS), precision=HIGH, preferred_element_type=jnp.float32)
    proj_re = cross[:NEV, :NRHS] + cross[NEV:, NRHS:]
    proj_im = cross[:NEV, NRHS:] - cross[NEV:, :NRHS]
    denom = (eig_real * eig_real + eig_imag * eig_imag)[:, None]
    coef_re = (proj_re * eig_real[:, None] + proj_im * eig_imag[:, None]) / denom
    coef_im = (proj_im * eig_real[:, None] - proj_re * eig_imag[:, None]) / denom
    block = jnp.concatenate([jnp.concatenate([coef_re, coef_im], 1), jnp.concatenate([-coef_im, coef_re], 1)], 0)
    solution = jnp.dot(rows, block, precision=HIGH, preferred_element_type=jnp.float32).reshape(rhs.shape)
    residual = rhs - operate(links, solution)
    for sweep in range(SWEEPS):
        image = operate(links, residual)
        swapped = jnp.concatenate([residual[..., NRHS:], residual[..., :NRHS]], -1)
        first = jnp.sum(image * residual, axis=(0, 1, 2, 3, 4))
        second = jnp.sum(image * swapped, axis=(0, 1, 2, 3, 4))
        power = jnp.sum(image * image, axis=(0, 1, 2, 3, 4))
        num_re = first[:NRHS] + first[NRHS:]
        num_im = second[:NRHS] - second[NRHS:]
        den = power[:NRHS] + power[NRHS:]
        alpha_re = num_re / den
        alpha_im = num_im / den
        solution = solution + complex_scale(alpha_re, alpha_im, residual)
        residual = residual - complex_scale(alpha_re, alpha_im, image)
    return solution, residual
```

```python
import math

import jax
import jax.numpy as jnp
from jax import lax
from jax.sharding import PartitionSpec as P

AXES = ("ta", "gz", "xy")
HIGH = lax.Precision.HIGHEST


def neighbours(x):
    forward, backward = [], []
    for dim, axis in enumerate(AXES):
        peers, length = lax.axis_size(axis), x.shape[dim]
        if peers == 1:
            forward.append(jnp.roll(x, -1, dim))
            backward.append(jnp.roll(x, 1, dim))
            continue
        up = [(i, (i + 1) % peers) for i in range(peers)]
        down = [(j, i) for i, j in up]
        first = lax.slice_in_dim(x, 0, 1, axis=dim)
        last = lax.slice_in_dim(x, length - 1, length, axis=dim)
        after = lax.ppermute(first, axis, down)
        before = after if peers == 2 and length == 1 else lax.ppermute(last, axis, up)
        if length > 1:
            after = jnp.concatenate([lax.slice_in_dim(x, 1, length, axis=dim), after], dim)
            before = jnp.concatenate([before, lax.slice_in_dim(x, 0, length - 1, axis=dim)], dim)
        forward.append(after)
        backward.append(before)
    forward.append(jnp.roll(x, -1, 3))
    backward.append(jnp.roll(x, 1, 3))
    return forward + backward


def fold(product, dof, half):
    top, low = product[..., :dof, :], product[..., dof:, :]
    parts = []
    for c in range(0, product.shape[-1], 2 * half):
        parts.append(top[..., c : c + half] - low[..., c + half : c + 2 * half])
        parts.append(top[..., c + half : c + 2 * half] + low[..., c : c + half])
    return jnp.concatenate(parts, -1)


def operate(matrix, field, half):
    dof = field.shape[4]
    stacked = jnp.concatenate([field] + neighbours(field), 4)
    product = jnp.einsum("tzxyok,tzxykc->tzxyoc", matrix, stacked, precision=HIGH)
    return fold(product, dof, half)


def reduce_doubling(x):
    for axis in reversed(AXES):
        peers = lax.axis_size(axis)
        if peers & (peers - 1):
            x = lax.psum(x, axis)
            continue
        bit = 1
        while bit < peers:
            x = x + lax.ppermute(x, axis, [(i, i ^ bit) for i in range(peers)])
            bit *= 2
    return x


def reduce_exchange(x):
    total = math.prod(lax.axis_size(a) for a in AXES)
    copies = jnp.broadcast_to(x[None], (total,) + x.shape)
    return jnp.sum(lax.all_to_all(copies, AXES, 0, 0, tiled=True), axis=0)


def swap(x, half):
    return jnp.concatenate([x[..., half:], x[..., :half]], -1)


def scale(alpha, x, half):
    re, im = alpha
    a = jnp.concatenate([re, re], -1)
    b = jnp.concatenate([-im, im], -1)
    return a * x + b * swap(x, half)


def products(k0, k1, k2, half):
    dims = tuple(range(k0.ndim - 1))
    s0, s1 = swap(k0, half), swap(k1, half)
    pairs = [(k1, k0), (k1, s0), (k2, k0), (k2, s0), (k2, k1), (k2, s1), (k1, k1), (k2, k2)]
    return jnp.stack([jnp.sum(a * b, axis=dims) for a, b in pairs])


def two_alphas(g, half):
    def inner(i):
        p, q = g[i], g[i + 1]
        return p[:half] + p[half:], q[:half] - q[half:]

    c10, c20, c21 = inner(0), inner(2), inner(4)
    n1, n2 = g[6][:half] + g[6][half:], g[7][:half] + g[7][half:]
    ar, ai = c10[0] / n1, c10[1] / n1
    a2 = ar * ar + ai * ai
    num_re = c10[0] - ar * n1 - (ar * c20[0] + ai * c20[1]) + a2 * c21[0]
    num_im = c10[1] - ai * n1 - (ar * c20[1] - ai * c20[0]) + a2 * c21[1]
    den = n1 - 2.0 * (ar * c21[0] + ai * c21[1]) + a2 * n2
    return (ar, ai), (num_re / den, num_im / den)


def local(links, eigvecs, eig_real, eig_imag, rhs):
    nev = eig_real.shape[0]
    half = rhs.shape[-1] // 2
    dof = rhs.shape[4]
    dirs = links.shape[4]
    lat = rhs.shape[:4]

    down = 2.0 ** -math.ceil(0.5 * math.log2(6 * dirs * dof))
    sign = jnp.where(jnp.arange(dirs) == 0, down, -down).astype(jnp.float32)
    matrix = links.reshape(lat + (dirs, dof, 2, dof)) * sign[:, None, None, None]
    matrix = matrix.transpose(0, 1, 2, 3, 6, 5, 4, 7).reshape(lat + (2 * dof, dirs * dof))

    rows = eigvecs.reshape(-1, 2 * nev)
    flat = rhs.reshape(-1, 2 * half)
    cross = jnp.dot(rows.T, flat, precision=HIGH, preferred_element_type=jnp.float32)
    proj = jnp.concatenate(
        [cross[:nev, :half] + cross[nev:, half:], cross[:nev, half:] - cross[nev:, :half]], 1
    )
    proj = reduce_doubling(proj)

    lifted = operate(matrix, eigvecs, nev)
    both = operate(matrix, jnp.concatenate([lifted, rhs], -1), half)

    proj_re, proj_im = proj[:, :half], proj[:, half:]
    denom = (eig_real * eig_real + eig_imag * eig_imag)[:, None]
    coef_re = (proj_re * eig_real[:, None] + proj_im * eig_imag[:, None]) / denom
    coef_im = (proj_im * eig_real[:, None] - proj_re * eig_imag[:, None]) / denom
    block = jnp.concatenate(
        [jnp.concatenate([coef_re, coef_im], 1), jnp.concatenate([-coef_im, coef_re], 1)], 0
    )
    up_block = block * (1.0 / down)

    def combine(field, weights):
        out = jnp.dot(
            field.reshape(-1, 2 * nev), weights, precision=HIGH, preferred_element_type=jnp.float32
        )
        return out.reshape(rhs.shape)

    start = combine(eigvecs, block)
    k0 = rhs - combine(lifted, up_block)
    k1 = both[..., 2 * nev :] - combine(both[..., : 2 * nev], up_block)
    k2 = operate(matrix, k1, half)
    gram = reduce_doubling(products(k0, k1, k2, half))
    k3 = operate(matrix, k2, half)
    k4 = operate(matrix, k3, half)
    a0, a1 = two_alphas(gram, half)

    def step(alpha, x, y):
        return x - scale(alpha, y, half)

    r1, s1, t1, u1 = (step(a0, x, y) for x, y in ((k0, k1), (k1, k2), (k2, k3), (k3, k4)))
    r2, s2, t2 = (step(a1, x, y) for x, y in ((r1, s1), (s1, t1), (t1, u1)))
    a2, a3 = two_alphas(reduce_exchange(products(r2, s2, t2, half)), half)
    r3, s3 = step(a2, r2, s2), step(a2, s2, t2)

    def grow(x, alpha, y):
        return x + down * scale(alpha, y, half)

    solution = grow(grow(grow(grow(start, a0, k0), a1, r1), a2, r2), a3, r3)
    return solution, step(a3, r3, s3)


def solution(mesh):
    field = P("ta", "gz", "xy", None, None, None)
    return jax.shard_map(
        local,
        mesh=mesh,
        in_specs=(field, field, P(), P(), field),
        out_specs=(field, field),
        check_vma=False,
    )
```

```python
import math

import jax
import jax.numpy as jnp
from jax import lax
from jax.sharding import PartitionSpec as P


AXES = ("ta", "gz", "xy")
HIGH = lax.Precision.HIGHEST
SWEEPS = 4


def split(x, dim):
    axis = AXES[dim]
    peers, length = lax.axis_size(axis), x.shape[dim]
    if peers == 1:
        return jnp.roll(x, -1, dim), jnp.roll(x, 1, dim)
    up = [(i, (i + 1) % peers) for i in range(peers)]
    down = [(j, i) for i, j in up]
    first = lax.slice_in_dim(x, 0, 1, axis=dim)
    last = lax.slice_in_dim(x, length - 1, length, axis=dim)
    before = lax.ppermute(last, axis, up)
    if peers == 2 and length == 1:
        return before, before
    after = lax.ppermute(first, axis, down)
    if length > 1:
        after = jnp.concatenate([lax.slice_in_dim(x, 1, length, axis=dim), after], dim)
        before = jnp.concatenate([before, lax.slice_in_dim(x, 0, length - 1, axis=dim)], dim)
    return after, before


def fold(product, dof, half):
    top, low = product[..., :dof, :], product[..., dof:, :]
    parts = []
    for c in range(0, product.shape[-1], 2 * half):
        parts.append(top[..., c : c + half] - low[..., c + half : c + 2 * half])
        parts.append(top[..., c + half : c + 2 * half] + low[..., c : c + half])
    return jnp.concatenate(parts, -1)


def operate(matrices, field, half):
    near, far = matrices
    dof = field.shape[4]
    (ta_next, ta_prev), (gz_next, gz_prev), (xy_next, xy_prev) = (split(field, d) for d in range(3))
    y_next, y_prev = jnp.roll(field, -1, 3), jnp.roll(field, 1, 3)
    close = jnp.concatenate([field, gz_next, xy_next, y_next, gz_prev, xy_prev, y_prev], 4)
    away = jnp.concatenate([ta_next, ta_prev], 4)
    product = jnp.einsum("tzxyok,tzxykc->tzxyoc", near, close, precision=HIGH)
    product = product + jnp.einsum("tzxyok,tzxykc->tzxyoc", far, away, precision=HIGH)
    return fold(product, dof, half)


def reduce_stages(x):
    total = math.prod(lax.axis_size(a) for a in AXES)
    bits = total.bit_length() - 1
    if total != 1 << bits:
        return lax.psum(x, AXES)
    low = 0
    while low < bits:
        width = 1 if low == 0 and bits % 2 else 2
        parts = [x]
        for mask in range(1, 1 << width):
            pairs = [(i, i ^ (mask << low)) for i in range(total)]
            parts.append(lax.ppermute(x, AXES, pairs))
        x = sum(parts[1:], parts[0])
        low += width
    return x


def reduce_exchange(x):
    total = math.prod(lax.axis_size(a) for a in AXES)
    copies = jnp.broadcast_to(x[None], (total,) + x.shape)
    return jnp.sum(lax.all_to_all(copies, AXES, 0, 0, tiled=True), axis=0)


def swap(x, half):
    return jnp.concatenate([x[..., half:], x[..., :half]], -1)


def scale(alpha, x, half):
    re, im = alpha
    a = jnp.concatenate([re, re], -1)
    b = jnp.concatenate([-im, im], -1)
    return a * x + b * swap(x, half)


def products(k0, k1, k2, half):
    dims = tuple(range(k0.ndim - 1))
    s0, s1 = swap(k0, half), swap(k1, half)
    pairs = [(k1, k0), (k1, s0), (k2, k0), (k2, s0), (k2, k1), (k2, s1), (k1, k1), (k2, k2)]
    return jnp.stack([jnp.sum(a * b, axis=dims) for a, b in pairs])


def two_alphas(g, half):
    def inner(i):
        p, q = g[i], g[i + 1]
        return p[:half] + p[half:], q[:half] - q[half:]

    c10, c20, c21 = inner(0), inner(2), inner(4)
    n1, n2 = g[6][:half] + g[6][half:], g[7][:half] + g[7][half:]
    ar, ai = c10[0] / n1, c10[1] / n1
    a2 = ar * ar + ai * ai
    num_re = c10[0] - ar * n1 - (ar * c20[0] + ai * c20[1]) + a2 * c21[0]
    num_im = c10[1] - ai * n1 - (ar * c20[1] - ai * c20[0]) + a2 * c21[1]
    den = n1 - 2.0 * (ar * c21[0] + ai * c21[1]) + a2 * n2
    return (ar, ai), (num_re / den, num_im / den)


def local(links, eigvecs, eig_real, eig_imag, rhs):
    nev = eig_real.shape[0]
    half = rhs.shape[-1] // 2
    dof = rhs.shape[4]
    dirs = links.shape[4]
    lat = rhs.shape[:4]

    down = 2.0 ** -math.ceil(0.5 * math.log2(6 * dirs * dof))
    sign = jnp.where(jnp.arange(dirs) == 0, down, -down).astype(jnp.float32)
    matrix = links.reshape(lat + (dirs, dof, 2, dof)) * sign[:, None, None, None]
    matrix = matrix.transpose(0, 1, 2, 3, 6, 5, 4, 7)

    def pick(which):
        chosen = jnp.concatenate([matrix[..., d : d + 1, :] for d in which], -2)
        return chosen.reshape(lat + (2 * dof, len(which) * dof))

    matrices = (pick((0, 2, 3, 4, 6, 7, 8)), pick((1, 5)))

    rows = eigvecs.reshape(-1, 2 * nev)
    flat = rhs.reshape(-1, 2 * half)
    cross = jnp.dot(rows.T, flat, precision=HIGH, preferred_element_type=jnp.float32)
    proj = jnp.concatenate(
        [cross[:nev, :half] + cross[nev:, half:], cross[:nev, half:] - cross[nev:, :half]], 1
    )
    proj = reduce_stages(proj)
    lifted = operate(matrices, eigvecs, nev)

    proj_re, proj_im = proj[:, :half], proj[:, half:]
    denom = (eig_real * eig_real + eig_imag * eig_imag)[:, None]
    coef_re = (proj_re * eig_real[:, None] + proj_im * eig_imag[:, None]) / denom
    coef_im = (proj_im * eig_real[:, None] - proj_re * eig_imag[:, None]) / denom
    block = jnp.concatenate(
        [jnp.concatenate([coef_re, coef_im], 1), jnp.concatenate([-coef_im, coef_re], 1)], 0
    )
    up_block = block * (1.0 / down)

    def combine(field, weights):
        out = jnp.dot(
            field.reshape(-1, 2 * nev), weights, precision=HIGH, preferred_element_type=jnp.float32
        )
        return out.reshape(rhs.shape)

    start = combine(eigvecs, block)
    k0 = rhs - combine(lifted, up_block)
    ks = [k0]
    for i in range(1, SWEEPS + 1):
        ks.append(operate(matrices, ks[-1], half))
        if i == 2:
            gram = reduce_exchange(products(*ks, half))
    k0, k1, k2, k3, k4 = ks
    a0, a1 = two_alphas(gram, half)

    def step(alpha, x, y):
        return x - scale(alpha, y, half)

    r1, s1, t1, u1 = (step(a0, x, y) for x, y in ((k0, k1), (k1, k2), (k2, k3), (k3, k4)))
    r2, s2, t2 = (step(a1, x, y) for x, y in ((r1, s1), (s1, t1), (t1, u1)))
    a2, a3 = two_alphas(reduce_exchange(products(r2, s2, t2, half)), half)
    r3, s3 = step(a2, r2, s2), step(a2, s2, t2)

    def grow(x, alpha, y):
        return x + down * scale(alpha, y, half)

    solution = grow(grow(grow(grow(start, a0, k0), a1, r1), a2, r2), a3, r3)
    return solution, step(a3, r3, s3)


def solution(mesh):
    field = P("ta", "gz", "xy", None, None, None)
    return jax.shard_map(
        local,
        mesh=mesh,
        in_specs=(field, field, P(), P(), field),
        out_specs=(field, field),
        check_vma=False,
    )
```
